256 devices in a mesh: groups: 4 (over x, y), tensor: 64 (over z, core).
Axes of the slice: x: 2, y: 2, z: 32, core: 2. Of those that a mesh axis runs over, the one named last changes fastest.
The devices are a block of a 4x8x32 slice.
Arguments:
- stem_field: float32 [16, 2, 1048576], P('groups', None, 'tensor'), parts along dimension 0, may hold values from -6 to 6
- branches: float32 [4, 2, 2, 256, 256], P(None, None, None, None, 'tensor'), may hold values from -0.25 to 0.25
- branch_order: int32 [4], replicated, may hold values from 0 to 3, each once
- slice_values: int32 [16, 4], P('groups'), parts along dimension 0, may hold values from 0 to 1
Outputs:
- amplitudes: float32 [8, 1048576], P('groups', 'tensor'), parts along dimension 0
The draws below stay inside these ranges and needn't reach their ends.
There are 4 independent parts, one for each index of `groups`. The reference program is written for one: setup_inputs(seed, part) draws one part's arguments, and reference() takes and returns one part's arrays. A program takes and returns all parts, laid end to end along the dimension named above; an argument that names none is the same for every part. Nothing has to cross between parts.
Inputs may be any that keep to these rules, and one draw needn't show every extreme that they name: `branch_order`: each branch is merged exactly once.
All inputs are finite; a program needn't handle non-finite values.
Results may differ from the reference program's by a relative error of at most 0.00014.
Values sent between devices are 32-bit elements; how exact they have to be, the bound alone decides.
No kernel may reach another device: no remote copies, remote signals or barrier semaphores. Data moves between devices by JAX's collectives and lax.ppermute only.
A program may use at most 64 MiB of HBM per device.

```python
import jax
import jax.numpy as jnp
from jax import lax

S = 4
STEPS = 4
CB = 256
Q_DEV = 16384
NQ = 1048576
N_TENSOR = 64


def plant(array, stream_key, low, top_value):
    shape = array.shape
    spot = [jax.random.randint(jax.random.fold_in(stream_key, axis), (), 0, shape[axis]) for axis in range(len(shape))]
    array = array.at[tuple(spot)].set(low)
    longest = shape.index(max(shape))
    spot[longest] = (spot[longest] + 1) % shape[longest]
    return array.at[tuple(spot)].set(top_value)


def steps_of(key, dims, split, smallest, largest):
    gain, own = 1.0, jax.random.fold_in(key, 6)
    for position, parts in split:
        heights = jnp.exp(jax.random.uniform(jax.random.fold_in(own, position), (parts,), jnp.float32, smallest / len(split), largest / len(split)))
        gain = gain * jnp.repeat(heights, dims[position] // parts).reshape([-1 if axis == position else 1 for axis in range(len(dims))])
    return gain


def centred(rng, dims, scale, limit, cuts=(), held_as=jnp.bfloat16):
    drawn = jax.random.normal(rng, dims, jnp.float32) * scale
    if len(cuts) > 0:
        drawn = steps_of(rng, dims, cuts, -0.22, 0.18) * drawn
    return jnp.clip(drawn, min=-limit, max=limit).astype(held_as)


def setup_inputs(seed: int = 0, part: int = 0) -> dict:
    key_of = jax.random.split(jax.random.key(seed), 5)
    part_splits = jax.random.split(jax.random.fold_in(key_of[4], part), 5)
    stem_field = centred(part_splits[0], (S, 2, NQ), 1.0, 6.0, ((2, 64),), jnp.float32)
    branches = centred(key_of[1], (STEPS, 2, 2, CB, CB), (2 * CB) ** -0.5, 0.25, ((4, 64),), jnp.float32)
    branch_order = jax.random.permutation(key_of[2], STEPS).astype(jnp.int32)
    slice_values = plant(jax.random.randint(part_splits[3], (S, STEPS), 0, 2), jax.random.fold_in(part_splits[3], 1), 0, 1).astype(jnp.int32)
    return {"stem_field": stem_field, "branches": branches, "branch_order": branch_order, "slice_values": slice_values}


def product(left, right):
    return jnp.einsum('shmi,sil->shml', left, right, precision=lax.Precision.HIGHEST)


def reference(stem_field, branches, branch_order, slice_values):
    shards = N_TENSOR
    middle = Q_DEV // CB
    current = stem_field
    for step_index in range(STEPS):
        branch_now = branches[branch_order[step_index]]
        values_now = slice_values[:, step_index]
        chosen = jnp.where((values_now == 1)[:, None, None, None], branch_now[1][None], branch_now[0][None])
        blocks = current.reshape(S, 2, shards, middle, CB)
        real_part = product(blocks[:, 0], chosen[:, 0]) - product(blocks[:, 1], chosen[:, 1])
        imag_part = product(blocks[:, 0], chosen[:, 1]) + product(blocks[:, 1], chosen[:, 0])
        combined = jnp.stack([real_part, imag_part], axis=1)
        combined = combined.reshape(S, 2, shards, middle, shards, CB // shards)
        current = combined.transpose(0, 1, 4, 2, 5, 3).reshape(S, 2, shards * Q_DEV)
    return jnp.sum(current, axis=0)
```

```python
import jax
import jax.numpy as jnp
from jax import lax
from jax.experimental import pallas as pl
from jax.experimental.pallas import tpu as pltpu
from jax.sharding import PartitionSpec as P

LANES = 128
HALF = LANES // 2
PRECISION = lax.Precision.HIGH


def dot_t(left, right):
    return lax.dot_general(
        left, right, (((1,), (1,)), ((), ())), precision=PRECISION, preferred_element_type=jnp.float32
    )


def dot(left, right):
    return lax.dot_general(
        left, right, (((1,), (0,)), ((), ())), precision=PRECISION, preferred_element_type=jnp.float32
    )


def low_lanes(rows):
    return lax.broadcasted_iota(jnp.int32, (rows, LANES), 1) < HALF


def put_table(table, piece, row, chips, parity, core):
    for value in range(2):
        at = row + 16 * value
        real, imag = piece[:, at : at + 8, :], piece[:, at + 8 : at + 16, :]
        low = lax.broadcasted_iota(jnp.int32, real.shape, 1) < 4
        real_r, imag_r = pltpu.roll(real, 4, 1), pltpu.roll(imag, 4, 1)
        columns = (
            jnp.where(low, real, imag_r),
            jnp.where(low, real_r, imag),
            jnp.where(low, -imag, real_r),
            jnp.where(low, -imag_r, real),
        )
        for spot, column in enumerate(columns):
            at = (4 * value + spot) * LANES
            table[chips, parity, core, :, at : at + LANES] = column


def put_tables(pieces, tables):
    place = lax.axis_index("tensor")
    core = lax.rem(place, 2)
    parity = lax.rem(place // 2, 2)
    chips = pieces[0].shape[0]
    for step, table in enumerate(tables):
        for (own, up, down), c in ((pieces[:3], core), (pieces[3:], 1 - core)):
            put_table(table, own, 32 * step, slice(0, chips), parity, c)
            put_table(table, up, 32 * step, slice(0, chips // 2), 1 - parity, c)
            put_table(table, down, 32 * step, slice(chips // 2, chips), 1 - parity, c)


def flat(table):
    return table[...].reshape(-1, table.shape[-1])


def put_rows(masked, x, row, column, chosen):
    rows, at, other = x.shape[0], column * LANES, (4 + column) * LANES
    zero = jnp.zeros_like(x)
    masked[row : row + rows, at : at + LANES] = jnp.where(chosen, zero, x)
    masked[row : row + rows, other : other + LANES] = jnp.where(chosen, x, zero)


def first_kernel(values, stem, *refs):
    pieces, (out, one, two, masked, state) = refs[:6], refs[6:]
    put_tables(pieces, (one, two))
    slices = values.shape[0]
    middle = stem.shape[0] // (4 * slices)
    for s in range(slices):
        for column in range(4):
            part, half = divmod(column, 2)
            x = stem[pl.ds(4 * middle * s + 2 * half + part, middle, stride=4), :]
            put_rows(masked, x, middle * s, column, values[s, 0] == 1)
    merged = dot_t(flat(one), masked[...])
    for pair in range(slices // 2):
        state[pair] = merged[:, pair * LANES : (pair + 1) * LANES]
    count = merged.shape[0] // 8
    low = low_lanes(count)
    for pair in range(slices // 2):
        for column in range(4):
            a = state[pair, pl.ds(2 * column, count, stride=8), :]
            b = state[pair, pl.ds(2 * column + 1, count, stride=8), :]
            even = jnp.where(low, a, pltpu.roll(b, HALF, 1))
            odd = jnp.where(low, pltpu.roll(a, HALF, 1), b)
            put_rows(masked, even, count * 2 * pair, column, values[2 * pair, 1] == 1)
            put_rows(masked, odd, count * (2 * pair + 1), column, values[2 * pair + 1, 1] == 1)
    merged = dot_t(flat(two), masked[...])
    for pair in range(slices // 2):
        x = merged[:, pair * LANES : (pair + 1) * LANES]
        out[:, 8 * pair : 8 * pair + 8, :] = x.reshape(count, 8, LANES)


def second_kernel(values, moved, *refs):
    pieces, (out, three, four, masked, sums, right, last) = refs[:6], refs[6:]
    put_tables(pieces, (three, four))
    slices = values.shape[0]
    pairs = slices // 2
    count = moved.shape[0] // (8 * pairs)
    low = low_lanes(count)

    def picked(pair, step, rows):
        in_low = low_lanes(rows)
        return (in_low & (values[2 * pair, step] == 1)) | (~in_low & (values[2 * pair + 1, step] == 1))

    for pair in range(pairs):
        at = pair * LANES
        one = picked(pair, 2, count)
        for j in range(8):
            x = moved[pl.ds(8 * pair + j, count, stride=8 * pairs), :]
            zero = jnp.zeros_like(x)
            masked[count * j : count * (j + 1), at : at + LANES] = jnp.where(one, zero, x)
            masked[count * (8 + j) : count * (9 + j), at : at + LANES] = jnp.where(one, x, zero)
    merged = dot(flat(three), masked[...])
    for value in range(2):
        total = jnp.zeros((merged.shape[0], LANES), jnp.float32)
        for pair in range(pairs):
            x = merged[:, pair * LANES : (pair + 1) * LANES]
            one = picked(pair, 3, merged.shape[0])
            total = total + (jnp.where(one, x, 0.0) if value else jnp.where(one, 0.0, x))
        sums[value] = total + pltpu.roll(total, HALF, 1)
    for value in range(2):
        for column in range(4):
            a = sums[value, pl.ds(2 * column, count, stride=8), :]
            b = sums[value, pl.ds(2 * column + 1, count, stride=8), :]
            x = jnp.where(low, a, b)
            at = (4 * value + column) * LANES
            right[0:count, at : at + LANES] = x
            right[count : 2 * count, at : at + LANES] = x
    last[...] = dot_t(flat(four), right[...])
    for column in range(4):
        a = last[pl.ds(2 * column, count, stride=8), :]
        b = last[pl.ds(2 * column + 1, count, stride=8), :]
        out[pl.ds(column, count, stride=4), :] = jnp.where(low, a, b)


def last_kernel(moved, out):
    count = moved.shape[0] // 4
    low = low_lanes(count)
    for part in range(2):
        rows = [moved[pl.ds(2 * part + half, count, stride=4), :] for half in range(2)]
        turned = jnp.concatenate(rows, axis=0).T
        first, second = turned[:count], turned[count:]
        out[pl.ds(part, count, stride=4), :] = jnp.where(low, first, pltpu.roll(second, HALF, 1))
        out[pl.ds(2 + part, count, stride=4), :] = jnp.where(low, pltpu.roll(first, HALF, 1), second)


def local_call(kernel, out_shape, scratch, n_scalars, n_inputs, flops):
    specs = [pl.BlockSpec(memory_space=pltpu.SMEM)] * n_scalars + [pl.BlockSpec(memory_space=pltpu.VMEM)] * n_inputs
    return pl.pallas_call(
        kernel,
        out_shape=jax.ShapeDtypeStruct(out_shape, jnp.float32),
        in_specs=specs,
        out_specs=pl.BlockSpec(memory_space=pltpu.VMEM),
        scratch_shapes=[pltpu.VMEM(shape, jnp.float32) for shape in scratch],
        cost_estimate=pl.CostEstimate(flops=flops, bytes_accessed=4 * 2**20, transcendentals=0),
        compiler_params=pltpu.CompilerParams(vmem_limit_bytes=24 * 2**20),
    )


def gather_same_core(block, shards):
    rings = [[core + 2 * (start + 2 * i) for i in range(shards // 4)] for start in range(2) for core in range(2)]
    return lax.all_gather(block, "tensor", axis_index_groups=rings)


def spread(own, shards):
    half = own.shape[0] // 2

    def send(x, chips, cross):
        pairs = [(i, ((i + 2 * chips) % shards) ^ cross) for i in range(shards)]
        return lax.ppermute(x, "tensor", pairs)

    lower, upper = own[:half], own[half:]
    return (own, send(lower, 1, 0), send(upper, -1, 0), send(own, 0, 1), send(lower, 1, 1), send(upper, -1, 1))


def per_device(stem_field, branches, branch_order, slice_values):
    shards = lax.axis_size("tensor")
    slices, parts, entries = stem_field.shape
    steps, n_values, _, contract, width = branches.shape
    middle = entries // contract
    halves = contract // LANES
    block = branches.transpose(0, 1, 2, 4, 3).reshape(steps, n_values, parts, width, halves, LANES)
    block = block.transpose(0, 1, 2, 4, 3, 5).reshape(steps, n_values * parts * halves * width, LANES)
    picked = [lax.dynamic_index_in_dim(block, branch_order[t], 0, keepdims=False) for t in range(steps)]
    stem = stem_field.reshape(slices, parts, middle * halves, LANES).transpose(0, 2, 1, 3).reshape(-1, LANES)
    first = gather_same_core(jnp.concatenate(picked[:2]), shards)
    later = gather_same_core(jnp.concatenate(picked[2:]), shards)
    first, later = spread(first, shards), spread(later, shards)

    rows = shards * 2 * width
    deep = n_values * parts * contract
    table = (shards // 4, 2, 2, 2 * width, deep)
    lanes = slices * middle
    flops = 2 * 2 * rows * deep * lanes
    merged = local_call(
        first_kernel,
        (shards, 8 * slices // 2, LANES),
        [table, table, (lanes, deep), (slices // 2, rows, LANES)],
        1,
        7,
        flops,
    )(slice_values, stem, *first)
    moved = lax.all_to_all(merged, "tensor", split_axis=0, concat_axis=0, tiled=True)
    summed = local_call(
        second_kernel,
        (shards * 4, LANES),
        [table, table, (deep, lanes), (2, rows, LANES), (2 * middle, deep), (rows, LANES)],
        1,
        7,
        flops,
    )(slice_values, moved.reshape(-1, LANES), *later)
    final = lax.all_to_all(summed.reshape(shards, 4, LANES), "tensor", split_axis=0, concat_axis=0, tiled=True)
    out = local_call(last_kernel, (middle * halves * parts, LANES), [], 0, 1, 1000)(final.reshape(-1, LANES))
    return out.reshape(middle * halves, parts, LANES).transpose(1, 0, 2).reshape(parts, entries)


def solution(mesh):
    return jax.shard_map(
        per_device,
        mesh=mesh,
        in_specs=(
            P("groups", None, "tensor"),
            P(None, None, None, None, "tensor"),
            P(),
            P("groups", None),
        ),
        out_specs=P("groups", "tensor"),
        check_vma=False,
    )
```

```python
import functools

import jax
import jax.numpy as jnp
from jax import lax
from jax.experimental import pallas as pl
from jax.experimental.pallas import tpu as pltpu
from jax.sharding import PartitionSpec as P


LANES = 128
HALF = LANES // 2
PRECISION = lax.Precision.HIGH


def dot_t(left, right):
    return lax.dot_general(
        left, right, (((1,), (1,)), ((), ())), precision=PRECISION, preferred_element_type=jnp.float32
    )


def dot(left, right):
    return lax.dot_general(
        left, right, (((1,), (0,)), ((), ())), precision=PRECISION, preferred_element_type=jnp.float32
    )


def low_lanes(rows):
    return lax.broadcasted_iota(jnp.int32, (rows, LANES), 1) < HALF


def put_table(table, piece, row, chips, parity, core):
    for value in range(2):
        at = row + 16 * value
        real, imag = piece[:, at : at + 8, :], piece[:, at + 8 : at + 16, :]
        low = lax.broadcasted_iota(jnp.int32, real.shape, 1) < 4
        real_r, imag_r = pltpu.roll(real, 4, 1), pltpu.roll(imag, 4, 1)
        columns = (
            jnp.where(low, real, imag_r),
            jnp.where(low, real_r, imag),
            jnp.where(low, -imag, real_r),
            jnp.where(low, -imag_r, real),
        )
        for spot, column in enumerate(columns):
            at = (4 * value + spot) * LANES
            table[chips, parity, core, :, at : at + LANES] = column


def put_tables(pieces, tables):
    place = lax.axis_index("tensor")
    core = lax.rem(place, 2)
    parity = lax.rem(place // 2, 2)
    chips = pieces[0].shape[0]
    for step, table in enumerate(tables):
        for (own, up, down), c in ((pieces[:3], core), (pieces[3:], 1 - core)):
            put_table(table, own, 32 * step, slice(0, chips), parity, c)
            put_table(table, up, 32 * step, slice(0, chips // 2), 1 - parity, c)
            put_table(table, down, 32 * step, slice(chips // 2, chips), 1 - parity, c)


def flat(table):
    return table[...].reshape(-1, table.shape[-1])


def put_rows(masked, x, row, column, chosen):
    rows, at, other = x.shape[0], column * LANES, (4 + column) * LANES
    zero = jnp.zeros_like(x)
    masked[row : row + rows, at : at + LANES] = jnp.where(chosen, zero, x)
    masked[row : row + rows, other : other + LANES] = jnp.where(chosen, x, zero)


def pick_kernel(first, order, block, after, out):
    rows = block.shape[1]
    for t in range(2):
        out[t * rows : (t + 1) * rows, :] = block[order[first + t]]


def first_kernel(values, stem, *refs):
    pieces, (after, out, one, two, masked, state) = refs[:6], refs[6:]
    put_tables(pieces, (one, two))
    slices = values.shape[0]
    middle = stem.shape[0] // (4 * slices)
    for s in range(slices):
        for column in range(4):
            part, half = divmod(column, 2)
            x = stem[pl.ds(4 * middle * s + 2 * half + part, middle, stride=4), :]
            put_rows(masked, x, middle * s, column, values[s, 0] == 1)
    merged = dot_t(flat(one), masked[...])
    for pair in range(slices // 2):
        state[pair] = merged[:, pair * LANES : (pair + 1) * LANES]
    count = merged.shape[0] // 8
    low = low_lanes(count)
    for pair in range(slices // 2):
        for column in range(4):
            a = state[pair, pl.ds(2 * column, count, stride=8), :]
            b = state[pair, pl.ds(2 * column + 1, count, stride=8), :]
            even = jnp.where(low, a, pltpu.roll(b, HALF, 1))
            odd = jnp.where(low, pltpu.roll(a, HALF, 1), b)
            put_rows(masked, even, count * 2 * pair, column, values[2 * pair, 1] == 1)
            put_rows(masked, odd, count * (2 * pair + 1), column, values[2 * pair + 1, 1] == 1)
    merged = dot_t(flat(two), masked[...])
    for pair in range(slices // 2):
        x = merged[:, pair * LANES : (pair + 1) * LANES]
        out[:, 8 * pair : 8 * pair + 8, :] = x.reshape(count, 8, LANES)


def table_kernel(*refs):
    put_tables(refs[:6], refs[6:])


def second_kernel(values, moved, three, four, out, masked, sums, right, last):
    slices = values.shape[0]
    pairs = slices // 2
    count = moved.shape[0] // (8 * pairs)
    low = low_lanes(count)

    def picked(pair, step, rows):
        in_low = low_lanes(rows)
        return (in_low & (values[2 * pair, step] == 1)) | (~in_low & (values[2 * pair + 1, step] == 1))

    for pair in range(pairs):
        at = pair * LANES
        one = picked(pair, 2, count)
        for j in range(8):
            x = moved[pl.ds(8 * pair + j, count, stride=8 * pairs), :]
            zero = jnp.zeros_like(x)
            masked[count * j : count * (j + 1), at : at + LANES] = jnp.where(one, zero, x)
            masked[count * (8 + j) : count * (9 + j), at : at + LANES] = jnp.where(one, x, zero)
    merged = dot(flat(three), masked[...])
    for value in range(2):
        total = jnp.zeros((merged.shape[0], LANES), jnp.float32)
        for pair in range(pairs):
            x = merged[:, pair * LANES : (pair + 1) * LANES]
            one = picked(pair, 3, merged.shape[0])
            total = total + (jnp.where(one, x, 0.0) if value else jnp.where(one, 0.0, x))
        sums[value] = total + pltpu.roll(total, HALF, 1)
    for value in range(2):
        for column in range(4):
            a = sums[value, pl.ds(2 * column, count, stride=8), :]
            b = sums[value, pl.ds(2 * column + 1, count, stride=8), :]
            x = jnp.where(low, a, b)
            at = (4 * value + column) * LANES
            right[0:count, at : at + LANES] = x
            right[count : 2 * count, at : at + LANES] = x
    last[...] = dot_t(flat(four), right[...])
    for column in range(4):
        a = last[pl.ds(2 * column, count, stride=8), :]
        b = last[pl.ds(2 * column + 1, count, stride=8), :]
        out[pl.ds(column, count, stride=4), :] = jnp.where(low, a, b)


def last_kernel(moved, out):
    count = moved.shape[0] // 4
    low = low_lanes(count)
    for part in range(2):
        rows = [moved[pl.ds(2 * part + half, count, stride=4), :] for half in range(2)]
        turned = jnp.concatenate(rows, axis=0).T
        first, second = turned[:count], turned[count:]
        out[pl.ds(part, count, stride=4), :] = jnp.where(low, first, pltpu.roll(second, HALF, 1))
        out[pl.ds(2 + part, count, stride=4), :] = jnp.where(low, pltpu.roll(first, HALF, 1), second)


def local_call(kernel, out_shape, scratch, spaces, flops):
    kinds = {"s": pltpu.SMEM, "v": pltpu.VMEM, "a": pl.ANY}
    specs = [pl.BlockSpec(memory_space=kinds[space]) for space in spaces]
    vmem = pl.BlockSpec(memory_space=pltpu.VMEM)
    many = isinstance(out_shape, list)
    shapes = [jax.ShapeDtypeStruct(shape, jnp.float32) for shape in (out_shape if many else [out_shape])]
    return pl.pallas_call(
        kernel,
        out_shape=shapes if many else shapes[0],
        in_specs=specs,
        out_specs=[vmem] * len(shapes) if many else vmem,
        scratch_shapes=[pltpu.VMEM(shape, jnp.float32) for shape in scratch],
        cost_estimate=pl.CostEstimate(flops=flops, bytes_accessed=4 * 2**20, transcendentals=0),
        compiler_params=pltpu.CompilerParams(vmem_limit_bytes=24 * 2**20),
    )


def gather_same_core(block, shards):
    rings = [[core + 2 * (start + 2 * i) for i in range(shards // 4)] for start in range(2) for core in range(2)]
    return lax.all_gather(block, "tensor", axis_index_groups=rings)


def spread(own, shards):
    half = own.shape[0] // 2
    lower, upper = own[:half], own[half:]
    sent = []
    for x, chips, cross in ((lower, 1, 0), (upper, -1, 0), (own, 0, 1), (lower, 1, 1), (upper, -1, 1)):
        pairs = [(i, ((i + 2 * chips) % shards) ^ cross) for i in range(shards)]
        sent.append(lax.ppermute(x, "tensor", pairs))
    return (own, *sent)


def per_device(stem_field, branches, branch_order, slice_values):
    shards = lax.axis_size("tensor")
    slices, parts, entries = stem_field.shape
    steps, n_values, _, contract, width = branches.shape
    middle = entries // contract
    halves = contract // LANES
    block = branches.transpose(0, 1, 2, 4, 3).reshape(steps, n_values, parts, width, halves, LANES)
    block = block.transpose(0, 1, 2, 4, 3, 5).reshape(steps, n_values * parts * halves * width, LANES)

    def pick(first, after):
        shape = (2 * block.shape[1], LANES)
        kernel = functools.partial(pick_kernel, first)
        return local_call(kernel, shape, [], "sva", 1000)(branch_order, block, after)

    stem = stem_field.reshape(slices, parts, middle * halves, LANES).transpose(0, 2, 1, 3).reshape(-1, LANES)
    first = gather_same_core(pick(0, slice_values), shards)
    later = gather_same_core(pick(2, first), shards)
    ordered = later
    first, later = spread(first, shards), spread(later, shards)

    rows = shards * 2 * width
    deep = n_values * parts * contract
    table = (shards // 4, 2, 2, 2 * width, deep)
    lanes = slices * middle
    flops = 2 * 2 * rows * deep * lanes
    merged = local_call(
        first_kernel,
        (shards, 8 * slices // 2, LANES),
        [table, table, (lanes, deep), (slices // 2, rows, LANES)],
        "svvvvvvva",
        flops,
    )(slice_values, stem, *first, ordered)
    moved = lax.all_to_all(merged, "tensor", split_axis=0, concat_axis=0, tiled=True)
    tables = local_call(table_kernel, [table, table], [], "vvvvvv", 1000)(*later)
    summed = local_call(
        second_kernel,
        (shards * 4, LANES),
        [(deep, lanes), (2, rows, LANES), (2 * middle, deep), (rows, LANES)],
        "svvv",
        flops,
    )(slice_values, moved.reshape(-1, LANES), *tables)
    final = lax.all_to_all(summed.reshape(shards, 4, LANES), "tensor", split_axis=0, concat_axis=0, tiled=True)
    out = local_call(last_kernel, (middle * halves * parts, LANES), [], "v", 1000)(final.reshape(-1, LANES))
    return out.reshape(middle * halves, parts, LANES).transpose(1, 0, 2).reshape(parts, entries)


def solution(mesh):
    return jax.shard_map(
        per_device,
        mesh=mesh,
        in_specs=(
            P("groups", None, "tensor"),
            P(None, None, None, None, "tensor"),
            P(),
            P("groups", None),
        ),
        out_specs=P("groups", "tensor"),
        check_vma=False,
    )
```

```python
import jax
import jax.numpy as jnp
from jax import lax
from jax.experimental import pallas as pl
from jax.experimental.pallas import tpu as pltpu
from jax.sharding import PartitionSpec as P


LANES = 128
HALF = LANES // 2
PRECISION = lax.Precision.HIGH


def dot_t(left, right):
    return lax.dot_general(
        left, right, (((1,), (1,)), ((), ())), precision=PRECISION, preferred_element_type=jnp.float32
    )


def dot(left, right):
    return lax.dot_general(
        left, right, (((1,), (0,)), ((), ())), precision=PRECISION, preferred_element_type=jnp.float32
    )


def low_lanes(rows):
    return lax.broadcasted_iota(jnp.int32, (rows, LANES), 1) < HALF


def put_table(table, piece, row, chips, parity, core):
    for value in range(2):
        at = row + 16 * value
        real, imag = piece[:, at : at + 8, :], piece[:, at + 8 : at + 16, :]
        low = lax.broadcasted_iota(jnp.int32, real.shape, 1) < 4
        real_r, imag_r = pltpu.roll(real, 4, 1), pltpu.roll(imag, 4, 1)
        columns = (
            jnp.where(low, real, imag_r),
            jnp.where(low, real_r, imag),
            jnp.where(low, -imag, real_r),
            jnp.where(low, -imag_r, real),
        )
        for spot, column in enumerate(columns):
            at = (4 * value + spot) * LANES
            table[chips, parity, core, :, at : at + LANES] = column


def core_and_parity():
    place = lax.axis_index("tensor")
    return lax.rem(place, 2), lax.rem(place // 2, 2)


def put_first(pieces, tables):
    core, parity = core_and_parity()
    chips = pieces[0].shape[0]
    for step, table in enumerate(tables):
        for (own, up, down), c in ((pieces[:3], core), (pieces[3:], 1 - core)):
            put_table(table, own, 32 * step, slice(0, chips), parity, c)
            put_table(table, up, 32 * step, slice(0, chips // 2), 1 - parity, c)
            put_table(table, down, 32 * step, slice(chips // 2, chips), 1 - parity, c)


def table_kernel(own, other, *tables):
    core, _ = core_and_parity()
    chips = own.shape[0]
    for step, table in enumerate(tables):
        for piece, c in ((own, core), (other, 1 - core)):
            for parity in range(2):
                put_table(table, piece.at[:, parity], 32 * step, slice(0, chips), parity, c)


def flat(table):
    return table[...].reshape(-1, table.shape[-1])


def put_rows(masked, x, row, column, chosen):
    rows, at, other = x.shape[0], column * LANES, (4 + column) * LANES
    zero = jnp.zeros_like(x)
    masked[row : row + rows, at : at + LANES] = jnp.where(chosen, zero, x)
    masked[row : row + rows, other : other + LANES] = jnp.where(chosen, x, zero)


def pick_kernel(order, block, *outs):
    rows = block.shape[1]
    for k, out in enumerate(outs):
        for t in range(2):
            out[t * rows : (t + 1) * rows, :] = block[order[2 * k + t]]


def first_kernel(values, stem, *refs):
    pieces, (out, one, two, masked, state) = refs[:6], refs[6:]
    put_first(pieces, (one, two))
    slices = values.shape[0]
    middle = stem.shape[0] // (4 * slices)
    for s in range(slices):
        for column in range(4):
            part, half = divmod(column, 2)
            x = stem[pl.ds(4 * middle * s + 2 * half + part, middle, stride=4), :]
            put_rows(masked, x, middle * s, column, values[s, 0] == 1)
    merged = dot_t(flat(one), masked[...])
    for pair in range(slices // 2):
        state[pair] = merged[:, pair * LANES : (pair + 1) * LANES]
    count = merged.shape[0] // 8
    low = low_lanes(count)
    for pair in range(slices // 2):
        for column in range(4):
            a = state[pair, pl.ds(2 * column, count, stride=8), :]
            b = state[pair, pl.ds(2 * column + 1, count, stride=8), :]
            even = jnp.where(low, a, pltpu.roll(b, HALF, 1))
            odd = jnp.where(low, pltpu.roll(a, HALF, 1), b)
            put_rows(masked, even, count * 2 * pair, column, values[2 * pair, 1] == 1)
            put_rows(masked, odd, count * (2 * pair + 1), column, values[2 * pair + 1, 1] == 1)
    merged = dot_t(flat(two), masked[...])
    for pair in range(slices // 2):
        x = merged[:, pair * LANES : (pair + 1) * LANES]
        out[:, 8 * pair : 8 * pair + 8, :] = x.reshape(count, 8, LANES)


def second_kernel(values, moved, three, four, out, masked, sums, right, last):
    slices = values.shape[0]
    pairs = slices // 2
    count = moved.shape[0] // (8 * pairs)
    low = low_lanes(count)

    def picked(pair, step, rows):
        in_low = low_lanes(rows)
        return (in_low & (values[2 * pair, step] == 1)) | (~in_low & (values[2 * pair + 1, step] == 1))

    for pair in range(pairs):
        at = pair * LANES
        one = picked(pair, 2, count)
        for j in range(8):
            x = moved[pl.ds(8 * pair + j, count, stride=8 * pairs), :]
            zero = jnp.zeros_like(x)
            masked[count * j : count * (j + 1), at : at + LANES] = jnp.where(one, zero, x)
            masked[count * (8 + j) : count * (9 + j), at : at + LANES] = jnp.where(one, x, zero)
    merged = dot(flat(three), masked[...])
    for value in range(2):
        total = jnp.zeros((merged.shape[0], LANES), jnp.float32)
        for pair in range(pairs):
            x = merged[:, pair * LANES : (pair + 1) * LANES]
            one = picked(pair, 3, merged.shape[0])
            total = total + (jnp.where(one, x, 0.0) if value else jnp.where(one, 0.0, x))
        sums[value] = total + pltpu.roll(total, HALF, 1)
    for value in range(2):
        for column in range(4):
            a = sums[value, pl.ds(2 * column, count, stride=8), :]
            b = sums[value, pl.ds(2 * column + 1, count, stride=8), :]
            x = jnp.where(low, a, b)
            at = (4 * value + column) * LANES
            right[0:count, at : at + LANES] = x
            right[count : 2 * count, at : at + LANES] = x
    last[...] = dot_t(flat(four), right[...])
    for column in range(4):
        a = last[pl.ds(2 * column, count, stride=8), :]
        b = last[pl.ds(2 * column + 1, count, stride=8), :]
        out[pl.ds(column, count, stride=4), :] = jnp.where(low, a, b)


def last_kernel(moved, out):
    count = moved.shape[0] // 4
    low = low_lanes(count)
    for part in range(2):
        rows = [moved[pl.ds(2 * part + half, count, stride=4), :] for half in range(2)]
        turned = jnp.concatenate(rows, axis=0).T
        first, second = turned[:count], turned[count:]
        out[pl.ds(part, count, stride=4), :] = jnp.where(low, first, pltpu.roll(second, HALF, 1))
        out[pl.ds(2 + part, count, stride=4), :] = jnp.where(low, pltpu.roll(first, HALF, 1), second)


def local_call(kernel, out_shape, scratch, spaces, flops):
    kinds = {"s": pltpu.SMEM, "v": pltpu.VMEM, "a": pl.ANY}
    specs = [pl.BlockSpec(memory_space=kinds[space]) for space in spaces]
    vmem = pl.BlockSpec(memory_space=pltpu.VMEM)
    many = isinstance(out_shape, list)
    shapes = [jax.ShapeDtypeStruct(shape, jnp.float32) for shape in (out_shape if many else [out_shape])]
    return pl.pallas_call(
        kernel,
        out_shape=shapes if many else shapes[0],
        in_specs=specs,
        out_specs=[vmem] * len(shapes) if many else vmem,
        scratch_shapes=[pltpu.VMEM(shape, jnp.float32) for shape in scratch],
        cost_estimate=pl.CostEstimate(flops=flops, bytes_accessed=4 * 2**20, transcendentals=0),
        compiler_params=pltpu.CompilerParams(vmem_limit_bytes=24 * 2**20),
    )


def send(x, shards, chips, cross):
    return lax.ppermute(x, "tensor", [(i, ((i + 2 * chips) % shards) ^ cross) for i in range(shards)])


def exchange(block, shards):
    rings = [[core + 2 * (start + 2 * i) for i in range(shards // 4)] for start in range(2) for core in range(2)]
    own = lax.all_gather(block, "tensor", axis_index_groups=rings)
    half = own.shape[0] // 2
    up, down = send(own[:half], shards, 1, 0), send(own[half:], shards, -1, 0)
    return own, up, down, send(own, shards, 0, 1), send(up, shards, 0, 1), send(down, shards, 0, 1)


def per_device(stem_field, branches, branch_order, slice_values):
    shards = lax.axis_size("tensor")
    slices, parts, entries = stem_field.shape
    steps, n_values, _, contract, width = branches.shape
    middle = entries // contract
    halves = contract // LANES
    block = branches.transpose(0, 1, 2, 4, 3).reshape(steps, n_values, parts, width, halves, LANES)
    block = block.transpose(0, 1, 2, 4, 3, 5).reshape(steps, n_values * parts * halves * width, LANES)

    stem = stem_field.reshape(slices, parts, middle * halves, LANES).transpose(0, 2, 1, 3).reshape(-1, LANES)
    picked = (2 * block.shape[1], LANES)
    first, later = local_call(pick_kernel, [picked, picked], [], "sv", 1000)(branch_order, block)
    cores = [[core + 2 * i for i in range(shards // 2)] for core in range(2)]
    later = lax.all_gather(later, "tensor", axis_index_groups=cores).reshape(shards // 4, 2, *picked)
    swapped = send(later, shards, 0, 1)
    first = exchange(first, shards)

    rows = shards * 2 * width
    deep = n_values * parts * contract
    table = (shards // 4, 2, 2, 2 * width, deep)
    lanes = slices * middle
    flops = 2 * 2 * rows * deep * lanes
    merged = local_call(
        first_kernel,
        (shards, 8 * slices // 2, LANES),
        [table, table, (lanes, deep), (slices // 2, rows, LANES)],
        "svvvvvvv",
        flops,
    )(slice_values, stem, *first)
    moved = lax.all_to_all(merged, "tensor", split_axis=0, concat_axis=0, tiled=True)
    tables = local_call(table_kernel, [table, table], [], "vv", 1000)(later, swapped)
    summed = local_call(
        second_kernel,
        (shards * 4, LANES),
        [(deep, lanes), (2, rows, LANES), (2 * middle, deep), (rows, LANES)],
        "svvv",
        flops,
    )(slice_values, moved.reshape(-1, LANES), *tables)
    final = lax.all_to_all(summed.reshape(shards, 4, LANES), "tensor", split_axis=0, concat_axis=0, tiled=True)
    out = local_call(last_kernel, (middle * halves * parts, LANES), [], "v", 1000)(final.reshape(-1, LANES))
    return out.reshape(middle * halves, parts, LANES).transpose(1, 0, 2).reshape(parts, entries)


def solution(mesh):
    return jax.shard_map(
        per_device,
        mesh=mesh,
        in_specs=(
            P("groups", None, "tensor"),
            P(None, None, None, None, "tensor"),
            P(),
            P("groups", None),
        ),
        out_specs=P("groups", "tensor"),
        check_vma=False,
    )
```

```python
import jax
import jax.numpy as jnp
from jax import lax
from jax.experimental import pallas as pl
from jax.experimental.pallas import tpu as pltpu
from jax.sharding import PartitionSpec as P


LANES = 128
HALF = LANES // 2
PRECISION = lax.Precision.HIGH


def dot_t(left, right):
    return lax.dot_general(
        left, right, (((1,), (1,)), ((), ())), precision=PRECISION, preferred_element_type=jnp.float32
    )


def dot(left, right):
    return lax.dot_general(
        left, right, (((1,), (0,)), ((), ())), precision=PRECISION, preferred_element_type=jnp.float32
    )


def low_lanes(rows):
    return lax.broadcasted_iota(jnp.int32, (rows, LANES), 1) < HALF


def put_table(table, piece, row, chips, parity, core):
    for value in range(2):
        at = row + 16 * value
        real, imag = piece[:, at : at + 8, :], piece[:, at + 8 : at + 16, :]
        low = lax.broadcasted_iota(jnp.int32, real.shape, 1) < 4
        real_r, imag_r = pltpu.roll(real, 4, 1), pltpu.roll(imag, 4, 1)
        columns = (
            jnp.where(low, real, imag_r),
            jnp.where(low, real_r, imag),
            jnp.where(low, -imag, real_r),
            jnp.where(low, -imag_r, real),
        )
        for spot, column in enumerate(columns):
            at = (4 * value + spot) * LANES
            table[chips, parity, core, :, at : at + LANES] = column


def core_and_parity():
    place = lax.axis_index("tensor")
    return lax.rem(place, 2), lax.rem(place // 2, 2)


def flat(table):
    return table[...].reshape(-1, table.shape[-1])


def put_rows(masked, x, row, column, flag):
    rows, at, other = x.shape[0], column * LANES, (4 + column) * LANES
    chosen = jnp.broadcast_to(flag, x.shape) == 1
    zero = jnp.zeros_like(x)
    masked[row : row + rows, at : at + LANES] = jnp.where(chosen, zero, x)
    masked[row : row + rows, other : other + LANES] = jnp.where(chosen, x, zero)


def pick_kernel(order_in, block_in, out, order, block, sems):
    copies = [
        pltpu.make_async_copy(order_in, order, sems.at[0]),
        pltpu.make_async_copy(block_in, block, sems.at[1]),
    ]
    for copy in copies:
        copy.start()
    for copy in copies:
        copy.wait()
    rows = block.shape[1]
    for k, t in enumerate((0, 1, 2 + turn())):
        out[k * rows : (k + 1) * rows, :] = block[order[t]]


def turn():
    return lax.rem(lax.axis_index("groups"), 2)


def core_and_parity():
    place = lax.axis_index("tensor")
    return lax.rem(place, 2), lax.rem(place // 2, 2)


def spots(pieces):
    core, parity = core_and_parity()
    chips = pieces[0].shape[0]
    for (own, up, down), c in ((pieces[:3], core), (pieces[3:], 1 - core)):
        yield own, slice(0, chips), parity, c
        yield up, slice(0, chips // 2), 1 - parity, c
        yield down, slice(chips // 2, chips), 1 - parity, c


def stem_kernel(values, stem, masked, flags):
    slices, steps = values.shape
    for t in range(steps):
        for s in range(slices):
            flags[t * slices + s : t * slices + s + 1, :] = jnp.full((1, LANES), values[s, t], jnp.int32)
        for pair in range(slices // 2):
            row = slices * steps + t * (slices // 2) + pair
            flags[row : row + 1, :] = jnp.where(low_lanes(1), values[2 * pair, t], values[2 * pair + 1, t])
    middle = stem.shape[0] // (4 * slices)
    for s in range(slices):
        for column in range(4):
            part, half = divmod(column, 2)
            x = stem[pl.ds(4 * middle * s + 2 * half + part, middle, stride=4), :]
            put_rows(masked, x, middle * s, column, flags[s : s + 1, :])


def first_kernel(flags, start, *refs):
    pieces, (out, mine, one, two, masked, state) = refs[:6], refs[6:]
    for piece, chips, parity, core in spots(pieces):
        for step, table in enumerate((one, two)):
            put_table(table, piece, 32 * step, chips, parity, core)
        mine[chips, parity, core] = piece[:, 64:, :]
    slices = out.shape[1] // 4
    merged = dot_t(flat(one), start[...])
    for pair in range(slices // 2):
        state[pair] = merged[:, pair * LANES : (pair + 1) * LANES]
    count = merged.shape[0] // 8
    low = low_lanes(count)
    for pair in range(slices // 2):
        for column in range(4):
            a = state[pair, pl.ds(2 * column, count, stride=8), :]
            b = state[pair, pl.ds(2 * column + 1, count, stride=8), :]
            even = jnp.where(low, a, pltpu.roll(b, HALF, 1))
            odd = jnp.where(low, pltpu.roll(a, HALF, 1), b)
            put_rows(masked, even, count * 2 * pair, column, flags[slices + 2 * pair : slices + 2 * pair + 1, :])
            put_rows(masked, odd, count * (2 * pair + 1), column, flags[slices + 2 * pair + 1 : slices + 2 * pair + 2, :])
    merged = dot_t(flat(two), masked[...])
    for pair in range(slices // 2):
        x = merged[:, pair * LANES : (pair + 1) * LANES]
        out[:, 8 * pair : 8 * pair + 8, :] = x.reshape(count, 8, LANES)


def second_kernel(flags, moved, mine, other, out, tables, masked, sums, right, last):
    for piece, spot in ((mine, turn()), (other, 1 - turn())):
        for k in range(4):
            parity, core = divmod(k, 2)
            put_table(tables.at[spot], piece.at[:, parity, core], 0, slice(0, piece.shape[0]), parity, core)
    three, four = tables.at[0], tables.at[1]
    pairs = masked.shape[1] // LANES
    count = moved.shape[0] // (8 * pairs)
    low = low_lanes(count)

    def picked(pair, step, rows):
        row = flags.shape[0] // 6 * 4 + step * pairs + pair
        return jnp.broadcast_to(flags[row : row + 1, :], (rows, LANES)) == 1

    for pair in range(pairs):
        at = pair * LANES
        one = picked(pair, 2, count)
        for j in range(8):
            x = moved[pl.ds(8 * pair + j, count, stride=8 * pairs), :]
            zero = jnp.zeros_like(x)
            masked[count * j : count * (j + 1), at : at + LANES] = jnp.where(one, zero, x)
            masked[count * (8 + j) : count * (9 + j), at : at + LANES] = jnp.where(one, x, zero)
    merged = dot(flat(three), masked[...])
    for value in range(2):
        total = jnp.zeros((merged.shape[0], LANES), jnp.float32)
        for pair in range(pairs):
            x = merged[:, pair * LANES : (pair + 1) * LANES]
            one = picked(pair, 3, merged.shape[0])
            total = total + (jnp.where(one, x, 0.0) if value else jnp.where(one, 0.0, x))
        sums[value] = total + pltpu.roll(total, HALF, 1)
    for value in range(2):
        for column in range(4):
            a = sums[value, pl.ds(2 * column, count, stride=8), :]
            b = sums[value, pl.ds(2 * column + 1, count, stride=8), :]
            x = jnp.where(low, a, b)
            at = (4 * value + column) * LANES
            right[0:count, at : at + LANES] = x
            right[count : 2 * count, at : at + LANES] = x
    last[...] = dot_t(flat(four), right[...])
    for column in range(4):
        a = last[pl.ds(2 * column, count, stride=8), :]
        b = last[pl.ds(2 * column + 1, count, stride=8), :]
        out[pl.ds(column, count, stride=4), :] = jnp.where(low, a, b)


def last_kernel(moved, out):
    count = moved.shape[0] // 4
    low = low_lanes(count)
    for part in range(2):
        rows = [moved[pl.ds(2 * part + half, count, stride=4), :] for half in range(2)]
        turned = jnp.concatenate(rows, axis=0).T
        first, second = turned[:count], turned[count:]
        out[pl.ds(part, count, stride=4), :] = jnp.where(low, first, pltpu.roll(second, HALF, 1))
        out[pl.ds(2 + part, count, stride=4), :] = jnp.where(low, pltpu.roll(first, HALF, 1), second)


def local_call(kernel, out_shape, scratch, spaces, flops, kinds_out=(jnp.float32,)):
    kinds = {"s": pltpu.SMEM, "v": pltpu.VMEM}
    specs = [pl.BlockSpec(memory_space=kinds[space]) for space in spaces]
    vmem = pl.BlockSpec(memory_space=pltpu.VMEM)
    many = isinstance(out_shape, list)
    shapes = [jax.ShapeDtypeStruct(*out) for out in zip(out_shape if many else [out_shape], kinds_out, strict=True)]
    return pl.pallas_call(
        kernel,
        out_shape=shapes if many else shapes[0],
        in_specs=specs,
        out_specs=[vmem] * len(shapes) if many else vmem,
        scratch_shapes=[pltpu.VMEM(shape, jnp.float32) for shape in scratch],
        cost_estimate=pl.CostEstimate(flops=flops, bytes_accessed=4 * 2**20, transcendentals=0),
        compiler_params=pltpu.CompilerParams(vmem_limit_bytes=24 * 2**20),
    )


def send(x, shards, chips, cross):
    return lax.ppermute(x, "tensor", [(i, ((i + 2 * chips) % shards) ^ cross) for i in range(shards)])


def exchange(block, shards):
    rings = [[core + 2 * (start + 2 * i) for i in range(shards // 4)] for start in range(2) for core in range(2)]
    own = lax.all_gather(block, "tensor", axis_index_groups=rings)
    half = own.shape[0] // 2
    up = send(own[:half], shards, 1, 0)
    down = send(own[half:], shards, -1, 0)
    return own, up, down, send(own, shards, 0, 1), send(up, shards, 0, 1), send(down, shards, 0, 1)


def per_device(stem_field, branches, branch_order, slice_values):
    shards = lax.axis_size("tensor")
    slices, parts, entries = stem_field.shape
    steps, n_values, _, contract, width = branches.shape
    middle = entries // contract
    halves = contract // LANES
    block = branches.transpose(0, 1, 2, 4, 3).reshape(steps, n_values, parts, width, halves, LANES)
    block = block.transpose(0, 1, 2, 4, 3, 5).reshape(steps, n_values * parts * halves * width, LANES)

    stem = stem_field.reshape(slices, parts, middle * halves, LANES).transpose(0, 2, 1, 3).reshape(-1, LANES)
    part_rows = block.shape[1]
    picked = pl.pallas_call(
        pick_kernel,
        out_shape=jax.ShapeDtypeStruct((3 * part_rows, LANES), jnp.float32),
        in_specs=[pl.BlockSpec(memory_space=pl.ANY)] * 2,
        out_specs=pl.BlockSpec(memory_space=pltpu.VMEM),
        scratch_shapes=[
            pltpu.SMEM((steps,), jnp.int32),
            pltpu.VMEM(block.shape, jnp.float32),
            pltpu.SemaphoreType.DMA((2,)),
        ],
    )(branch_order, block)
    pieces = exchange(picked, shards)

    rows = shards * 2 * width
    deep = n_values * parts * contract
    table = (shards // 4, 2, 2, 2 * width, deep)
    lanes = slices * middle
    flops = 2 * 2 * rows * deep * lanes
    pairs = slices // 2
    start, flags = local_call(
        stem_kernel, [(lanes, deep), ((slices + pairs) * steps, LANES)], [], "sv", 10**8, (jnp.float32, jnp.int32)
    )(slice_values, stem)
    merged, mine = local_call(
        first_kernel,
        [(shards, 8 * pairs, LANES), (shards // 4, 2, 2, part_rows, LANES)],
        [table, table, (lanes, deep), (pairs, rows, LANES)],
        "v" * 8,
        flops,
        (jnp.float32, jnp.float32),
    )(flags, start, *pieces)
    moved = lax.all_to_all(merged, "tensor", split_axis=0, concat_axis=0, tiled=True)
    other = lax.ppermute(mine, "groups", [(g, g ^ 1) for g in range(lax.axis_size("groups"))])
    summed = local_call(
        second_kernel,
        (shards * 4, LANES),
        [(2, *table), (deep, lanes), (2, rows, LANES), (2 * middle, deep), (rows, LANES)],
        "vvvv",
        flops,
    )(flags, moved.reshape(-1, LANES), mine, other)
    final = lax.all_to_all(summed.reshape(shards, 4, LANES), "tensor", split_axis=0, concat_axis=0, tiled=True)
    out = local_call(last_kernel, (middle * halves * parts, LANES), [], "v", 1000)(final.reshape(-1, LANES))
    return out.reshape(middle * halves, parts, LANES).transpose(1, 0, 2).reshape(parts, entries)


def solution(mesh):
    return jax.shard_map(
        per_device,
        mesh=mesh,
        in_specs=(
            P("groups", None, "tensor"),
            P(None, None, None, None, "tensor"),
            P(),
            P("groups", None),
        ),
        out_specs=P("groups", "tensor"),
        check_vma=False,
    )
```

```python
import jax
import jax.numpy as jnp
from jax import lax
from jax.experimental import pallas as pl
from jax.experimental.pallas import tpu as pltpu
from jax.sharding import PartitionSpec as P


LANES = 128
HALF = LANES // 2


def split(x):
    high = x.astype(jnp.bfloat16)
    return high, (x - high.astype(jnp.float32)).astype(jnp.bfloat16)


def product(left, right, axis):
    left_high, left_low = split(left)
    right_high, right_low = split(right)
    return lax.dot_general(
        jnp.concatenate([left_high, left_high, left_low], axis=1),
        jnp.concatenate([right_high, right_low, right_high], axis=axis),
        (((1,), (axis,)), ((), ())),
        preferred_element_type=jnp.float32,
    )


def low_lanes(rows):
    return lax.broadcasted_iota(jnp.int32, (rows, LANES), 1) < HALF


def put_table(table, piece, row, chips, parity, core):
    real, imag = piece[:, row : row + 8, :], piece[:, row + 8 : row + 16, :]
    low = lax.broadcasted_iota(jnp.int32, real.shape, 1) < 4
    real_r, imag_r = pltpu.roll(real, 4, 1), pltpu.roll(imag, 4, 1)
    columns = (
        jnp.where(low, real, imag_r),
        jnp.where(low, real_r, imag),
        jnp.where(low, -imag, real_r),
        jnp.where(low, -imag_r, real),
    )
    for spot, column in enumerate(columns):
        table[chips, parity, core, :, spot * LANES : (spot + 1) * LANES] = column


def flat(table):
    return jnp.concatenate([table[value].reshape(-1, table.shape[-1]) for value in range(2)], axis=1)


def put_rows(masked, x, row, column, flag):
    rows, at, other = x.shape[0], column * LANES, (4 + column) * LANES
    chosen = jnp.broadcast_to(flag, x.shape) == 1
    zero = jnp.zeros_like(x)
    masked[row : row + rows, at : at + LANES] = jnp.where(chosen, zero, x)
    masked[row : row + rows, other : other + LANES] = jnp.where(chosen, x, zero)


def pick_kernel(order_in, block_in, out, order, block, sems):
    copies = [
        pltpu.make_async_copy(order_in, order, sems.at[0]),
        pltpu.make_async_copy(block_in, block, sems.at[1]),
    ]
    for copy in copies:
        copy.start()
    for copy in copies:
        copy.wait()
    table, value = turn()
    for k, (t, v) in enumerate(((0, 0), (0, 1), (1, 0), (1, 1), (2 + table, value))):
        out[16 * k : 16 * (k + 1), :] = block[order[t], v]


def turn():
    quarter = lax.rem(lax.axis_index("groups"), 4)
    return quarter // 2, lax.rem(quarter, 2)


def core_and_parity():
    place = lax.axis_index("tensor")
    return lax.rem(place, 2), lax.rem(place // 2, 2)


def spots(pieces):
    core, parity = core_and_parity()
    chips = pieces[0].shape[0]
    for (own, up, down), c in ((pieces[:3], core), (pieces[3:], 1 - core)):
        yield own, slice(0, chips), parity, c
        yield up, slice(0, chips // 2), 1 - parity, c
        yield down, slice(chips // 2, chips), 1 - parity, c


def stem_kernel(values, stem, masked, flags):
    slices, steps = values.shape
    for t in range(steps):
        for s in range(slices):
            flags[t * slices + s : t * slices + s + 1, :] = jnp.full((1, LANES), values[s, t], jnp.int32)
        for pair in range(slices // 2):
            row = slices * steps + t * (slices // 2) + pair
            flags[row : row + 1, :] = jnp.where(low_lanes(1), values[2 * pair, t], values[2 * pair + 1, t])
    middle = stem.shape[0] // (4 * slices)
    for s in range(slices):
        for column in range(4):
            part, half = divmod(column, 2)
            x = stem[pl.ds(4 * middle * s + 2 * half + part, middle, stride=4), :]
            put_rows(masked, x, middle * s, column, flags[s : s + 1, :])


def first_kernel(flags, start, *refs):
    pieces, (out, mine, one, two, masked, state) = refs[:6], refs[6:]
    for piece, chips, parity, core in spots(pieces):
        for step, table in enumerate((one, two)):
            for value in range(2):
                put_table(table.at[value], piece, 32 * step + 16 * value, chips, parity, core)
        mine[chips, parity, core] = piece[:, 64:, :]
    slices = out.shape[1] // 4
    merged = product(flat(one), start[...], 1)
    for pair in range(slices // 2):
        state[pair] = merged[:, pair * LANES : (pair + 1) * LANES]
    count = merged.shape[0] // 8
    low = low_lanes(count)
    for pair in range(slices // 2):
        for column in range(4):
            a = state[pair, pl.ds(2 * column, count, stride=8), :]
            b = state[pair, pl.ds(2 * column + 1, count, stride=8), :]
            even = jnp.where(low, a, pltpu.roll(b, HALF, 1))
            odd = jnp.where(low, pltpu.roll(a, HALF, 1), b)
            put_rows(masked, even, count * 2 * pair, column, flags[slices + 2 * pair : slices + 2 * pair + 1, :])
            put_rows(masked, odd, count * (2 * pair + 1), column, flags[slices + 2 * pair + 1 : slices + 2 * pair + 2, :])
    merged = product(flat(two), masked[...], 1)
    for pair in range(slices // 2):
        x = merged[:, pair * LANES : (pair + 1) * LANES]
        out[:, 8 * pair : 8 * pair + 8, :] = x.reshape(count, 8, LANES)


def second_kernel(flags, moved, *refs):
    quarters, (out, tables, masked, sums, right, last) = refs[:4], refs[4:]
    table, value = turn()
    for k, piece in enumerate(quarters):
        spot = tables.at[(1 - table) if k % 2 else table, (1 - value) if k // 2 else value]
        for parity in range(2):
            for core in range(2):
                put_table(spot, piece.at[:, parity, core], 0, slice(0, piece.shape[0]), parity, core)
    three, four = tables.at[0], tables.at[1]
    pairs = masked.shape[1] // LANES
    count = moved.shape[0] // (8 * pairs)
    low = low_lanes(count)

    def picked(pair, step, rows):
        row = flags.shape[0] // 6 * 4 + step * pairs + pair
        return jnp.broadcast_to(flags[row : row + 1, :], (rows, LANES)) == 1

    for pair in range(pairs):
        at = pair * LANES
        one = picked(pair, 2, count)
        for j in range(8):
            x = moved[pl.ds(8 * pair + j, count, stride=8 * pairs), :]
            zero = jnp.zeros_like(x)
            masked[count * j : count * (j + 1), at : at + LANES] = jnp.where(one, zero, x)
            masked[count * (8 + j) : count * (9 + j), at : at + LANES] = jnp.where(one, x, zero)
    merged = product(flat(three), masked[...], 0)
    for value in range(2):
        total = jnp.zeros((merged.shape[0], LANES), jnp.float32)
        for pair in range(pairs):
            x = merged[:, pair * LANES : (pair + 1) * LANES]
            one = picked(pair, 3, merged.shape[0])
            total = total + (jnp.where(one, x, 0.0) if value else jnp.where(one, 0.0, x))
        sums[value] = total + pltpu.roll(total, HALF, 1)
    for value in range(2):
        for column in range(4):
            a = sums[value, pl.ds(2 * column, count, stride=8), :]
            b = sums[value, pl.ds(2 * column + 1, count, stride=8), :]
            x = jnp.where(low, a, b)
            at = (4 * value + column) * LANES
            right[0:count, at : at + LANES] = x
            right[count : 2 * count, at : at + LANES] = x
    last[...] = product(flat(four), right[...], 1)
    for column in range(4):
        a = last[pl.ds(2 * column, count, stride=8), :]
        b = last[pl.ds(2 * column + 1, count, stride=8), :]
        out[pl.ds(column, count, stride=4), :] = jnp.where(low, a, b)


def last_kernel(moved, out):
    count = moved.shape[0] // 4
    low = low_lanes(count)
    for part in range(2):
        rows = [moved[pl.ds(2 * part + half, count, stride=4), :] for half in range(2)]
        turned = jnp.concatenate(rows, axis=0).T
        first, second = turned[:count], turned[count:]
        out[pl.ds(part, count, stride=4), :] = jnp.where(low, first, pltpu.roll(second, HALF, 1))
        out[pl.ds(2 + part, count, stride=4), :] = jnp.where(low, pltpu.roll(first, HALF, 1), second)


def local_call(kernel, out_shape, scratch, spaces, flops, kinds_out=(jnp.float32,)):
    kinds = {"s": pltpu.SMEM, "v": pltpu.VMEM}
    specs = [pl.BlockSpec(memory_space=kinds[space]) for space in spaces]
    vmem = pl.BlockSpec(memory_space=pltpu.VMEM)
    many = isinstance(out_shape, list)
    shapes = [jax.ShapeDtypeStruct(*out) for out in zip(out_shape if many else [out_shape], kinds_out, strict=True)]
    return pl.pallas_call(
        kernel,
        out_shape=shapes if many else shapes[0],
        in_specs=specs,
        out_specs=[vmem] * len(shapes) if many else vmem,
        scratch_shapes=[pltpu.VMEM(shape, jnp.float32) for shape in scratch],
        cost_estimate=pl.CostEstimate(flops=flops, bytes_accessed=4 * 2**20, transcendentals=0),
        compiler_params=pltpu.CompilerParams(vmem_limit_bytes=24 * 2**20),
    )


def send(x, shards, chips, cross):
    return lax.ppermute(x, "tensor", [(i, ((i + 2 * chips) % shards) ^ cross) for i in range(shards)])


def exchange(block, shards):
    rings = [[core + 2 * (start + 2 * i) for i in range(shards // 4)] for start in range(2) for core in range(2)]
    own = lax.all_gather(block, "tensor", axis_index_groups=rings)
    half = own.shape[0] // 2
    up = send(own[:half], shards, 1, 0)
    down = send(own[half:], shards, -1, 0)
    return own, up, down, send(own, shards, 0, 1), send(up, shards, 0, 1), send(down, shards, 0, 1)


def per_device(stem_field, branches, branch_order, slice_values):
    shards = lax.axis_size("tensor")
    slices, parts, entries = stem_field.shape
    steps, n_values, _, contract, width = branches.shape
    middle = entries // contract
    halves = contract // LANES
    block = branches.transpose(0, 1, 2, 4, 3).reshape(steps, n_values, parts, width, halves, LANES)
    block = block.transpose(0, 1, 2, 4, 3, 5).reshape(steps, n_values, -1, LANES)

    stem = stem_field.reshape(slices, parts, middle * halves, LANES).transpose(0, 2, 1, 3).reshape(-1, LANES)
    part_rows = parts * halves * width
    picked = pl.pallas_call(
        pick_kernel,
        out_shape=jax.ShapeDtypeStruct((5 * part_rows, LANES), jnp.float32),
        in_specs=[pl.BlockSpec(memory_space=pl.ANY)] * 2,
        out_specs=pl.BlockSpec(memory_space=pltpu.VMEM),
        scratch_shapes=[
            pltpu.SMEM((steps,), jnp.int32),
            pltpu.VMEM(block.shape, jnp.float32),
            pltpu.SemaphoreType.DMA((2,)),
        ],
    )(branch_order, block)
    pieces = exchange(picked, shards)

    rows = shards * 2 * width
    deep = n_values * parts * contract
    table = (n_values, shards // 4, 2, 2, 2 * width, parts * contract)
    lanes = slices * middle
    flops = 2 * 2 * rows * deep * lanes
    pairs = slices // 2
    start, flags = local_call(
        stem_kernel, [(lanes, deep), ((slices + pairs) * steps, LANES)], [], "sv", 10**8, (jnp.float32, jnp.int32)
    )(slice_values, stem)
    merged, mine = local_call(
        first_kernel,
        [(shards, 8 * pairs, LANES), (shards // 4, 2, 2, part_rows, LANES)],
        [table, table, (lanes, deep), (pairs, rows, LANES)],
        "v" * 8,
        flops,
        (jnp.float32, jnp.float32),
    )(flags, start, *pieces)
    moved = lax.all_to_all(merged, "tensor", split_axis=0, concat_axis=0, tiled=True)
    groups = lax.axis_size("groups")

    def trade(x, bit):
        return lax.ppermute(x, "groups", [(g, g ^ bit) for g in range(groups)])

    other = trade(mine, 2)
    quarters = (mine, other, trade(mine, 1), trade(other, 1))
    summed = local_call(
        second_kernel,
        (shards * 4, LANES),
        [(2, *table), (deep, lanes), (2, rows, LANES), (2 * middle, deep), (rows, LANES)],
        "v" * 6,
        flops,
    )(flags, moved.reshape(-1, LANES), *quarters)
    final = lax.all_to_all(summed.reshape(shards, 4, LANES), "tensor", split_axis=0, concat_axis=0, tiled=True)
    out = local_call(last_kernel, (middle * halves * parts, LANES), [], "v", 1000)(final.reshape(-1, LANES))
    return out.reshape(middle * halves, parts, LANES).transpose(1, 0, 2).reshape(parts, entries)


def solution(mesh):
    return jax.shard_map(
        per_device,
        mesh=mesh,
        in_specs=(
            P("groups", None, "tensor"),
            P(None, None, None, None, "tensor"),
            P(),
            P("groups", None),
        ),
        out_specs=P("groups", "tensor"),
        check_vma=False,
    )
```
